32 devices in a mesh: grp: 4 (over y, x), dev: 8 (over z, core).
Axes of the slice: x: 2, y: 2, z: 4, core: 2. Of those that a mesh axis runs over, the one named last changes fastest.
Arguments:
- embeddings: bfloat16 [262144, 256], P(('grp', 'dev'))
- prior_dist: float32 [262144], P(('grp', 'dev')), may hold values from 1 to 3
- seed_ids: int32 [6, 512], replicated, may hold values from 0 to 262143, as said below
Outputs:
- min_dist: float32 [262144], P(('grp', 'dev'))
- group_means: float32 [6, 4], P(None, 'grp')
The draws below stay inside these ranges and needn't reach their ends.
Inputs may be any that keep to these rules, and one draw needn't show every extreme that they name: `seed_ids`: round r's ids all lie in the rows of group r mod 4, that is from (r mod 4) * 65536 to (r mod 4 + 1) * 65536 - 1; ids may repeat.
All inputs are finite; a program needn't handle non-finite values.
Results may differ from the reference program's by a relative error of at most 0.0003.
Values may be sent and summed in bfloat16 or wider, within the bound.
A program may use at most 64 MiB of HBM per device.

```python
import jax
import jax.numpy as jnp
from jax import lax

W = 256
SEEDS = 512
ROUNDS = 6
ROW_DEV = 8192
GROUP_ROWS = 65536
ROWS = 262144
GROUPS = 4


def draw_embeddings(key, part):
    key_rows, key_scale, key_shift, key_center, key_member = jax.random.split(jax.random.fold_in(key, 11), 5)
    cluster_count = 4 * SEEDS
    member = jax.random.randint(key_member, (ROWS,), 0, cluster_count, dtype=jnp.int32)
    centroids = jax.random.normal(key_center, (cluster_count, W), jnp.float32)
    scales = jnp.exp(jax.random.uniform(key_scale, (cluster_count,), jnp.float32, -0.7, 0.7))
    row_scale = jnp.take(scales, member, axis=0)
    row_center = jnp.take(centroids, member, axis=0)
    noise = jax.random.normal(key_rows, (ROWS, W), jnp.float32)
    values = row_scale[:, None] * (row_center + 0.3 * noise)
    return values.astype(jnp.bfloat16)


def draw_seed_ids(key, part):
    owners = jnp.arange(ROUNDS, dtype=jnp.int32) % GROUPS
    within = jax.random.randint(jax.random.fold_in(key, 23), (ROUNDS, SEEDS), 0, GROUP_ROWS, dtype=jnp.int32)
    return (owners[:, None] * GROUP_ROWS + within).astype(jnp.int32)


def steps_of(own_key, extent, cuts, least, top_value):
    factor_of = 1.0
    for position, blocks in cuts:
        steps = jax.random.uniform(jax.random.fold_in(jax.random.fold_in(own_key, 6), position), (blocks,), jnp.float32, least / len(cuts), top_value / len(cuts))
        factor_of = factor_of * jnp.repeat(jnp.exp(steps), extent[position] // blocks).reshape((-1,) + (1,) * (len(extent) - 1 - position))
    return factor_of


def setup_inputs(seed: int = 0) -> dict:
    key_of = jax.random.split(jax.random.key(seed), 4)
    return {
        "embeddings": draw_embeddings(jax.random.fold_in(key_of[3], 71), 0),
        "prior_dist": jnp.clip(1.0 + 2.0 * jax.random.uniform(key_of[1], (ROWS,), jnp.float32) ** steps_of(key_of[1], (ROWS,), ((0, 32),), -0.2, 0.2), 1.0, 3.0),
        "seed_ids": draw_seed_ids(jax.random.fold_in(key_of[3], 71), 0),
    }


def block_nearest(block, block_norms, centers, seed_norms):
    products = jnp.dot(block, centers.T, preferred_element_type=jnp.float32)
    gaps = jnp.maximum(block_norms[:, None] + seed_norms[None, :] - 2.0 * products, 0.0) / float(W)
    return jnp.min(gaps, axis=1)


def reference(embeddings, prior_dist, seed_ids):
    row_norms = jnp.sum(jnp.square(embeddings.astype(jnp.float32)), axis=1)
    block_count = ROWS // ROW_DEV
    blocks = embeddings.reshape(block_count, ROW_DEV, W)
    norm_blocks = row_norms.reshape(block_count, ROW_DEV)
    current = prior_dist
    means = []
    for round_index in range(ROUNDS):
        centers = jnp.take(embeddings, seed_ids[round_index], axis=0)
        seed_norms = jnp.sum(jnp.square(centers.astype(jnp.float32)), axis=1)

        def one_block(pair):
            return block_nearest(pair[0], pair[1], centers, seed_norms)

        nearest = lax.map(one_block, (blocks, norm_blocks)).reshape(ROWS)
        current = jnp.minimum(current, nearest)
        means.append(jnp.sum(current.reshape(GROUPS, GROUP_ROWS), axis=1) / float(GROUP_ROWS))
    return current, jnp.stack(means)
```

```python
import functools

import jax
import jax.numpy as jnp
from jax import lax
from jax.experimental import pallas as pl
from jax.experimental.pallas import tpu as pltpu
from jax.sharding import PartitionSpec as P

MESH = pl.DeviceIdType.MESH
LOAD_CHUNKS = 8
TILE = 256
NT = (((1,), (1,)), ((), ()))


def split_square(x):
    square = jnp.square(x)
    high = square.astype(jnp.bfloat16)
    return high, (square - high.astype(jnp.float32)).astype(jnp.bfloat16)


def kernel(
    sizes, ids, prior, e_hbm, dist, means,
    e, ef, pick, out_half, own_half, pin, half, zin, cent, snb, hm, rn, part, parts,
    load_sem, p_sem, rs_sem, ag_sem, grp_sem, fwd_sem, mean_sem,
):
    groups, devs, rounds, seeds, rows, width = sizes
    chips = devs // 2
    half_rows = seeds // 2
    piece = half_rows // chips
    slots = (rounds + groups - 1) // groups
    g, d = lax.axis_index("grp"), lax.axis_index("dev")
    c, h = d // 2, d % 2
    partner = c * 2 + (1 - h)
    row_start = (g * devs + d) * rows
    chunk = rows // LOAD_CHUNKS

    def load(i):
        at = pl.ds(i * chunk, chunk)
        return pltpu.make_async_copy(e_hbm.at[at], e.at[at], load_sem.at[i])

    for i in range(LOAD_CHUNKS):
        load(i).start()

    barrier = pltpu.get_barrier_semaphore()
    for o in range(1, devs):
        pl.semaphore_signal(barrier, inc=1, device_id=(g, (d + o) % devs), device_id_type=MESH)

    def peer(o):
        total, base = 0, 1
        while base < groups:
            total = total + (((g // base) % 2 + (o // base) % 2) % 2) * base
            base *= 2
        return total

    for o in range(1, groups):
        pl.semaphore_signal(barrier, inc=1, device_id=(peer(o), d), device_id_type=MESH)

    for i in range(LOAD_CHUNKS):
        load(i).wait()

        @pl.loop(0, chunk // 64)
        def _(t):
            at = pl.ds(pl.multiple_of(i * chunk + t * 64, 64), 64)
            ef[at, :] = e[at, :].astype(jnp.float32)

    def gather(slot, which, dst):
        r = g + groups * slot

        @pl.loop(0, half_rows // 16)
        def _(b):
            for q in range(16):
                i = b * 16 + q
                offset = ids[r, which * half_rows + i] - row_start
                inside = (offset >= 0) & (offset < rows)
                row = ef[pl.ds(jnp.where(inside, offset, 0), 1), :]
                pick[pl.ds(i, 1), :] = jnp.where(inside, row, 0.0)

        dst[slot] = pick[0:half_rows, :].astype(jnp.bfloat16)

    def send(src, dst, sem, k, j, device):
        return pltpu.make_async_remote_copy(
            src_ref=src, dst_ref=dst, send_sem=sem.at[0, k, j], recv_sem=sem.at[1, k, j],
            device_id=device, device_id_type=MESH,
        )

    def to_partner(k):
        return send(out_half.at[k], pin.at[k], p_sem, k, 0, (g, partner))

    def scatter(k, o):
        target = (c + o) % chips
        return send(half.at[k, target], zin.at[k, o], rs_sem, k, o, (g, target * 2 + h))

    def spread(k, o):
        block = cent.at[g + groups * k, h, c]
        return send(block, block, ag_sem, k, o, (g, ((c + o) % chips) * 2 + h))

    def across(k, o, origin=None):
        block = cent.at[(g if origin is None else origin) + groups * k, h]
        return send(block, block, grp_sem, k, o, (peer(o), d))

    def forward(k, o):
        block = cent.at[peer(o) + groups * k, h]
        return send(block, block, fwd_sem, k, o, (g, partner))

    def if_held(k, o, f):
        if groups * (k + 1) <= rounds:
            f()
        else:
            pl.when(peer(o) + groups * k < rounds)(f)

    first = True
    for k in range(slots):
        def start_slot(k=k, first=first):
            gather(k, 1 - h, out_half)
            if first:
                pl.semaphore_wait(barrier, devs - 1 + groups - 1)
            to_partner(k).start()
            gather(k, h, own_half)

        if_held(k, 0, start_slot)
        first = False

    for k in range(slots):
        def reduce_pair(k=k):
            to_partner(k).wait_recv()
            both = own_half[k] + pin[k]
            half[k] = both.reshape(chips, piece, width)
            for o in range(1, chips):
                scatter(k, o).start()

        if_held(k, 0, reduce_pair)

    ones_row = jnp.ones((8, width), jnp.bfloat16)

    @pl.loop(0, rows // TILE)
    def _(t):
        at = pl.ds(pl.multiple_of(t * TILE, TILE), TILE)
        high, low = split_square(ef[at, :])
        total = lax.dot_general(ones_row, high, NT, preferred_element_type=jnp.float32)
        total += lax.dot_general(ones_row, low, NT, preferred_element_type=jnp.float32)
        for q in range(TILE // 128):
            rn[t * (TILE // 128) + q] = total[:, q * 128 : (q + 1) * 128]

    for k in range(slots):
        def reduce_chips(k=k):
            total = half[k, c]
            for o in range(1, chips):
                scatter(k, o).wait_recv()
                total += zin[k, o]
            cent[g + groups * k, h, c] = total
            for o in range(1, chips):
                spread(k, o).start()

        if_held(k, 0, reduce_chips)

    for k in range(slots):
        def share(k=k):
            for o in range(1, chips):
                spread(k, o).wait_recv()
            for o in range(1, groups):
                across(k, o).start()
            forward(k, 0).start()

        if_held(k, 0, share)

    ones_col = jnp.ones((width, 128), jnp.bfloat16)

    def compute(r):
        centers = cent[r].reshape(seeds, width)
        high, low = split_square(centers.astype(jnp.float32))
        norms = jnp.dot(high, ones_col, preferred_element_type=jnp.float32)
        norms += jnp.dot(low, ones_col, preferred_element_type=jnp.float32)
        snb[...] = 0.5 * norms

        @pl.loop(0, rows // TILE)
        def _(t):
            at = pl.multiple_of(t * TILE, TILE)
            block = e[pl.ds(at, TILE), :]
            products = lax.dot_general(
                cent[r].reshape(seeds, width), block, NT, preferred_element_type=jnp.float32
            )
            for q in range(TILE // 128):
                score = products[:, q * 128 : (q + 1) * 128] - snb[...]
                hm[r, t * (TILE // 128) + q] = jnp.max(score.reshape(seeds // 8, 8, 128), axis=0)

    items = [(k, o) for k in range(slots) for o in range(groups)]

    def relay(k, o):
        def f():
            across(k, o, peer(o)).wait_recv()
            forward(k, o).start()

        if o:
            if_held(k, o, f)

    def finish(k, o):
        def f():
            forward(k, o).wait_recv()
            compute(peer(o) + groups * k)

        if_held(k, o, f)

    for n, (k, o) in enumerate(items):
        if n + 1 < len(items):
            relay(*items[n + 1])
        finish(k, o)

    current = prior[...]
    norms = jnp.max(rn[...], axis=1)
    sums = []
    for r in range(rounds):
        best = jnp.max(hm[r], axis=1)
        gap = jnp.maximum(norms - 2.0 * best, 0.0) * (1.0 / width)
        current = jnp.minimum(current, gap)
        sums.append(jnp.sum(current, axis=0, keepdims=True))
    if rounds < 8:
        sums.append(jnp.zeros((8 - rounds, 128), jnp.float32))
    part[...] = jnp.concatenate(sums, axis=0)
    dist[...] = current

    def send_part(o):
        return send(part, parts.at[o], mean_sem, 0, o, (g, (d + o) % devs))

    for o in range(1, devs):
        send_part(o).start()
    total = part[...]
    for o in range(1, devs):
        send_part(o).wait_recv()
        total += parts[o]
    means[...] = jnp.broadcast_to(
        jnp.sum(total, axis=1, keepdims=True) / float(rows * devs), (8, 128)
    )

    for o in range(1, devs):
        send_part(o).wait_send()
    for k in range(slots):
        def drain(k=k):
            to_partner(k).wait_send()
            for o in range(1, chips):
                scatter(k, o).wait_send()
                spread(k, o).wait_send()
            for o in range(1, groups):
                across(k, o).wait_send()

        if_held(k, 0, drain)
        for o in range(groups):
            if_held(k, o, lambda k=k, o=o: forward(k, o).wait_send())


def body(embeddings, prior_dist, seed_ids):
    rows, width = embeddings.shape
    rounds, seeds = seed_ids.shape
    groups, devs = lax.axis_size("grp"), lax.axis_size("dev")
    chips = devs // 2
    slots = (rounds + groups - 1) // groups
    half_rows = seeds // 2
    piece = half_rows // chips
    bf16, f32 = jnp.bfloat16, jnp.float32
    vmem = pl.BlockSpec(memory_space=pltpu.VMEM)
    dist, means = pl.pallas_call(
        functools.partial(kernel, (groups, devs, rounds, seeds, rows, width)),
        out_shape=(
            jax.ShapeDtypeStruct((rows // 128, 128), f32),
            jax.ShapeDtypeStruct((8, 128), f32),
        ),
        in_specs=[
            pl.BlockSpec(memory_space=pltpu.SMEM),
            vmem,
            pl.BlockSpec(memory_space=pl.ANY),
        ],
        out_specs=(vmem, vmem),
        scratch_shapes=[
            pltpu.VMEM((rows, width), bf16),
            pltpu.VMEM((rows + 8, width), f32),
            pltpu.VMEM((half_rows + 8, width), f32),
            pltpu.VMEM((slots, half_rows, width), bf16),
            pltpu.VMEM((slots, half_rows, width), bf16),
            pltpu.VMEM((slots, half_rows, width), bf16),
            pltpu.VMEM((slots, chips, piece, width), bf16),
            pltpu.VMEM((slots, chips, piece, width), bf16),
            pltpu.VMEM((rounds, 2, chips, piece, width), bf16),
            pltpu.VMEM((seeds, 128), f32),
            pltpu.VMEM((rounds, rows // 128, 8, 128), f32),
            pltpu.VMEM((rows // 128, 8, 128), f32),
            pltpu.VMEM((8, 128), f32),
            pltpu.VMEM((devs, 8, 128), f32),
            pltpu.SemaphoreType.DMA((LOAD_CHUNKS,)),
            pltpu.SemaphoreType.DMA((2, slots, 1)),
            pltpu.SemaphoreType.DMA((2, slots, chips)),
            pltpu.SemaphoreType.DMA((2, slots, chips)),
            pltpu.SemaphoreType.DMA((2, slots, groups)),
            pltpu.SemaphoreType.DMA((2, slots, groups)),
            pltpu.SemaphoreType.DMA((2, 1, devs)),
        ],
        compiler_params=pltpu.CompilerParams(
            collective_id=0, has_side_effects=True, vmem_limit_bytes=56 * 1024 * 1024
        ),
        name="seed_rounds",
    )(seed_ids, prior_dist.reshape(rows // 128, 128), embeddings)
    return dist.reshape(rows), means[:rounds, :1]


def solution(mesh):
    placed = (P(("grp", "dev"), None), P(("grp", "dev")), P())
    return jax.shard_map(
        body,
        mesh=mesh,
        in_specs=placed,
        out_specs=(P(("grp", "dev")), P(None, "grp")),
        check_vma=False,
    )
```

```python
import functools

import jax
import jax.numpy as jnp
from jax import lax
from jax.experimental import pallas as pl
from jax.experimental.pallas import tpu as pltpu
from jax.sharding import PartitionSpec as P

MESH = pl.DeviceIdType.MESH
LOAD_CHUNKS = 8
TILE = 256
WIDE = 2048
NT = (((1,), (1,)), ((), ()))


def split_square(x):
    square = jnp.square(x)
    high = square.astype(jnp.bfloat16)
    return high, (square - high.astype(jnp.float32)).astype(jnp.bfloat16)


def kernel(
    sizes, ids, prior, e_hbm, dist, means,
    e, ef, pick, out_half, own_half, pin, half, zin, cent, snb, hm, rn, part, parts,
    load_sem, p_sem, rs_sem, ag_sem, grp_sem, fwd_sem, mean_sem,
):
    groups, devs, rounds, seeds, rows, width = sizes
    chips = devs // 2
    half_rows = seeds // 2
    piece = half_rows // chips
    slots = (rounds + groups - 1) // groups
    g, d = lax.axis_index("grp"), lax.axis_index("dev")
    c, h = d // 2, d % 2
    partner = c * 2 + (1 - h)
    row_start = (g * devs + d) * rows
    chunk = rows // LOAD_CHUNKS

    def load(i):
        at = pl.ds(i * chunk, chunk)
        return pltpu.make_async_copy(e_hbm.at[at], e.at[at], load_sem.at[i])

    for i in range(LOAD_CHUNKS):
        load(i).start()

    barrier = pltpu.get_barrier_semaphore()
    for o in range(1, devs):
        pl.semaphore_signal(barrier, inc=1, device_id=(g, (d + o) % devs), device_id_type=MESH)

    def peer(o):
        total, base = 0, 1
        while base < groups:
            total = total + (((g // base) % 2 + (o // base) % 2) % 2) * base
            base *= 2
        return total

    for o in range(1, groups):
        pl.semaphore_signal(barrier, inc=1, device_id=(peer(o), d), device_id_type=MESH)

    for i in range(LOAD_CHUNKS):
        load(i).wait()

        @pl.loop(0, chunk // 64)
        def _(t):
            at = pl.ds(pl.multiple_of(i * chunk + t * 64, 64), 64)
            ef[at, :] = e[at, :].astype(jnp.float32)

    def gather(slot, which, dst):
        r = g + groups * slot

        @pl.loop(0, half_rows // 16)
        def _(b):
            for q in range(16):
                i = b * 16 + q
                offset = ids[r, which * half_rows + i] - row_start
                inside = (offset >= 0) & (offset < rows)
                row = ef[pl.ds(jnp.where(inside, offset, 0), 1), :]
                pick[pl.ds(i, 1), :] = jnp.where(inside, row, 0.0)

        dst[slot] = pick[0:half_rows, :].astype(jnp.bfloat16)

    def send(src, dst, sem, k, j, device):
        return pltpu.make_async_remote_copy(
            src_ref=src, dst_ref=dst, send_sem=sem.at[0, k, j], recv_sem=sem.at[1, k, j],
            device_id=device, device_id_type=MESH,
        )

    def to_partner(k):
        return send(out_half.at[k], pin.at[k], p_sem, k, 0, (g, partner))

    def scatter(k, o):
        target = (c + o) % chips
        return send(half.at[k, target], zin.at[k, o], rs_sem, k, o, (g, target * 2 + h))

    def spread(k, o):
        block = cent.at[g + groups * k, h, c]
        return send(block, block, ag_sem, k, o, (g, ((c + o) % chips) * 2 + h))

    def across(k, o, origin=None):
        block = cent.at[(g if origin is None else origin) + groups * k, h]
        return send(block, block, grp_sem, k, o, (peer(o), d))

    def forward(k, o):
        block = cent.at[peer(o) + groups * k, h]
        return send(block, block, fwd_sem, k, o, (g, partner))

    def if_held(k, o, f):
        if groups * (k + 1) <= rounds:
            f()
        else:
            pl.when(peer(o) + groups * k < rounds)(f)

    first = True
    for k in range(slots):
        def start_slot(k=k, first=first):
            gather(k, 1 - h, out_half)
            if first:
                pl.semaphore_wait(barrier, devs - 1 + groups - 1)
            to_partner(k).start()
            gather(k, h, own_half)

        if_held(k, 0, start_slot)
        first = False

    for k in range(slots):
        def reduce_pair(k=k):
            to_partner(k).wait_recv()
            both = own_half[k] + pin[k]
            half[k] = both.reshape(chips, piece, width)
            for o in range(1, chips):
                scatter(k, o).start()

        if_held(k, 0, reduce_pair)

    ones_row = jnp.ones((8, width), jnp.bfloat16)

    @pl.loop(0, rows // WIDE)
    def _(t):
        for j in range(WIDE // TILE):
            high, low = split_square(ef[pl.ds(pl.multiple_of(t * WIDE + j * TILE, TILE), TILE), :])
            total = lax.dot_general(ones_row, high, NT, preferred_element_type=jnp.float32)
            total += lax.dot_general(ones_row, low, NT, preferred_element_type=jnp.float32)
            for q in range(TILE // 128):
                at = t * (WIDE // 128) + j * (TILE // 128) + q
                rn[at] = total[:, q * 128 : (q + 1) * 128]

    for k in range(slots):
        def reduce_chips(k=k):
            total = half[k, c]
            for o in range(1, chips):
                scatter(k, o).wait_recv()
                total += zin[k, o]
            cent[g + groups * k, h, c] = total
            for o in range(1, chips):
                spread(k, o).start()

        if_held(k, 0, reduce_chips)

    for k in range(slots):
        def share(k=k):
            for o in range(1, chips):
                spread(k, o).wait_recv()
            for o in range(1, groups):
                across(k, o).start()
            forward(k, 0).start()

        if_held(k, 0, share)

    ones_col = jnp.ones((width, 128), jnp.bfloat16)

    def compute(r):
        centers = cent[r].reshape(seeds, width)
        high, low = split_square(centers.astype(jnp.float32))
        norms = jnp.dot(high, ones_col, preferred_element_type=jnp.float32)
        norms += jnp.dot(low, ones_col, preferred_element_type=jnp.float32)
        snb[...] = 0.5 * norms

        @pl.loop(0, rows // WIDE)
        def _(t):
            for j in range(WIDE // TILE):
                at = pl.multiple_of(t * WIDE + j * TILE, TILE)
                products = lax.dot_general(
                    cent[r].reshape(seeds, width), e[pl.ds(at, TILE), :], NT,
                    preferred_element_type=jnp.float32,
                )
                for q in range(TILE // 128):
                    score = products[:, q * 128 : (q + 1) * 128] - snb[...]
                    hm[r, t * (WIDE // 128) + j * (TILE // 128) + q] = jnp.max(
                        score.reshape(seeds // 8, 8, 128), axis=0
                    )

    items = [(k, o) for k in range(slots) for o in range(groups)]

    def relay(k, o):
        def f():
            across(k, o, peer(o)).wait_recv()
            forward(k, o).start()

        if o:
            if_held(k, o, f)

    def finish(k, o):
        def f():
            forward(k, o).wait_recv()
            compute(peer(o) + groups * k)

        if_held(k, o, f)

    for n, (k, o) in enumerate(items):
        if n + 1 < len(items):
            relay(*items[n + 1])
        finish(k, o)

    current = prior[...]
    norms = jnp.max(rn[...], axis=1)
    sums = []
    for r in range(rounds):
        best = jnp.max(hm[r], axis=1)
        gap = jnp.maximum(norms - 2.0 * best, 0.0) * (1.0 / width)
        current = jnp.minimum(current, gap)
        sums.append(jnp.sum(current, axis=0, keepdims=True))
    if rounds < 8:
        sums.append(jnp.zeros((8 - rounds, 128), jnp.float32))
    part[...] = jnp.concatenate(sums, axis=0)
    dist[...] = current

    def send_part(o):
        return send(part, parts.at[o], mean_sem, 0, o, (g, (d + o) % devs))

    for o in range(1, devs):
        send_part(o).start()
    total = part[...]
    for o in range(1, devs):
        send_part(o).wait_recv()
        total += parts[o]
    means[...] = jnp.broadcast_to(
        jnp.sum(total, axis=1, keepdims=True) / float(rows * devs), (8, 128)
    )

    for o in range(1, devs):
        send_part(o).wait_send()
    for k in range(slots):
        def drain(k=k):
            to_partner(k).wait_send()
            for o in range(1, chips):
                scatter(k, o).wait_send()
                spread(k, o).wait_send()
            for o in range(1, groups):
                across(k, o).wait_send()

        if_held(k, 0, drain)
        for o in range(groups):
            if_held(k, o, lambda k=k, o=o: forward(k, o).wait_send())


def body(embeddings, prior_dist, seed_ids):
    rows, width = embeddings.shape
    rounds, seeds = seed_ids.shape
    groups, devs = lax.axis_size("grp"), lax.axis_size("dev")
    chips = devs // 2
    slots = (rounds + groups - 1) // groups
    half_rows = seeds // 2
    piece = half_rows // chips
    bf16, f32 = jnp.bfloat16, jnp.float32
    vmem = pl.BlockSpec(memory_space=pltpu.VMEM)
    dist, means = pl.pallas_call(
        functools.partial(kernel, (groups, devs, rounds, seeds, rows, width)),
        out_shape=(
            jax.ShapeDtypeStruct((rows // 128, 128), f32),
            jax.ShapeDtypeStruct((8, 128), f32),
        ),
        in_specs=[
            pl.BlockSpec(memory_space=pltpu.SMEM),
            vmem,
            pl.BlockSpec(memory_space=pl.ANY),
        ],
        out_specs=(vmem, vmem),
        scratch_shapes=[
            pltpu.VMEM((rows, width), bf16),
            pltpu.VMEM((rows + 8, width), f32),
            pltpu.VMEM((half_rows + 8, width), f32),
            pltpu.VMEM((slots, half_rows, width), bf16),
            pltpu.VMEM((slots, half_rows, width), bf16),
            pltpu.VMEM((slots, half_rows, width), bf16),
            pltpu.VMEM((slots, chips, piece, width), bf16),
            pltpu.VMEM((slots, chips, piece, width), bf16),
            pltpu.VMEM((rounds, 2, chips, piece, width), bf16),
            pltpu.VMEM((seeds, 128), f32),
            pltpu.VMEM((rounds, rows // 128, 8, 128), f32),
            pltpu.VMEM((rows // 128, 8, 128), f32),
            pltpu.VMEM((8, 128), f32),
            pltpu.VMEM((devs, 8, 128), f32),
            pltpu.SemaphoreType.DMA((LOAD_CHUNKS,)),
            pltpu.SemaphoreType.DMA((2, slots, 1)),
            pltpu.SemaphoreType.DMA((2, slots, chips)),
            pltpu.SemaphoreType.DMA((2, slots, chips)),
            pltpu.SemaphoreType.DMA((2, slots, groups)),
            pltpu.SemaphoreType.DMA((2, slots, groups)),
            pltpu.SemaphoreType.DMA((2, 1, devs)),
        ],
        compiler_params=pltpu.CompilerParams(
            collective_id=0, has_side_effects=True, vmem_limit_bytes=56 * 1024 * 1024
        ),
        name="seed_rounds",
    )(seed_ids, prior_dist.reshape(rows // 128, 128), embeddings)
    return dist.reshape(rows), means[:rounds, :1]


def solution(mesh):
    placed = (P(("grp", "dev"), None), P(("grp", "dev")), P())
    return jax.shard_map(
        body,
        mesh=mesh,
        in_specs=placed,
        out_specs=(P(("grp", "dev")), P(None, "grp")),
        check_vma=False,
    )
```

```python
import functools

import jax
import jax.numpy as jnp
from jax import lax
from jax.experimental import pallas as pl
from jax.experimental.pallas import tpu as pltpu
from jax.sharding import PartitionSpec as P

MESH = pl.DeviceIdType.MESH
LOAD_CHUNKS = 8
TILE = 256
WIDE = 2048
NT = (((1,), (1,)), ((), ()))


def split_square(x):
    square = jnp.square(x)
    high = square.astype(jnp.bfloat16)
    return high, (square - high.astype(jnp.float32)).astype(jnp.bfloat16)


def kernel(
    sizes, ids, prior, e_hbm, dist, means,
    e, ef, pick, out_half, own_half, pin, half, zin, cent, snb, hm, rn, part, parts,
    load_sem, p_sem, rs_sem, ag_sem, grp_sem, fwd_sem, mean_sem,
):
    groups, devs, rounds, seeds, rows, width = sizes
    chips = devs // 2
    half_rows = seeds // 2
    piece = half_rows // chips
    slots = (rounds + groups - 1) // groups
    g, d = lax.axis_index("grp"), lax.axis_index("dev")
    c, h = d // 2, d % 2
    partner = c * 2 + (1 - h)
    row_start = (g * devs + d) * rows
    chunk = rows // LOAD_CHUNKS

    def load(i):
        at = pl.ds(i * chunk, chunk)
        return pltpu.make_async_copy(e_hbm.at[at], e.at[at], load_sem.at[i])

    for i in range(LOAD_CHUNKS):
        load(i).start()

    barrier = pltpu.get_barrier_semaphore()
    for o in range(1, devs):
        pl.semaphore_signal(barrier, inc=1, device_id=(g, (d + o) % devs), device_id_type=MESH)

    def peer(o):
        total, base = 0, 1
        while base < groups:
            total = total + (((g // base) % 2 + (o // base) % 2) % 2) * base
            base *= 2
        return total

    for o in range(1, groups):
        pl.semaphore_signal(barrier, inc=1, device_id=(peer(o), d), device_id_type=MESH)

    for i in range(LOAD_CHUNKS):
        load(i).wait()

        @pl.loop(0, chunk // 256)
        def _(t):
            at = pl.ds(pl.multiple_of(i * chunk + t * 256, 256), 256)
            ef[at, :] = e[at, :].astype(jnp.float32)

    def gather(slot, which, dst):
        r = g + groups * slot

        @pl.loop(0, half_rows // 16)
        def _(b):
            for q in range(16):
                i = b * 16 + q
                offset = ids[r, which * half_rows + i] - row_start
                inside = (offset >= 0) & (offset < rows)
                row = ef[pl.ds(jnp.where(inside, offset, 0), 1), :]
                pick[pl.ds(i, 1), :] = jnp.where(inside, row, 0.0)

        dst[slot] = pick[0:half_rows, :].astype(jnp.bfloat16)

    def send(src, dst, sem, k, j, device):
        return pltpu.make_async_remote_copy(
            src_ref=src, dst_ref=dst, send_sem=sem.at[0, k, j], recv_sem=sem.at[1, k, j],
            device_id=device, device_id_type=MESH,
        )

    def to_partner(k):
        return send(out_half.at[k], pin.at[k], p_sem, k, 0, (g, partner))

    def scatter(k, o):
        target = (c + o) % chips
        return send(half.at[k, target], zin.at[k, o], rs_sem, k, o, (g, target * 2 + h))

    def spread(k, o):
        block = cent.at[g + groups * k, h, c]
        return send(block, block, ag_sem, k, o, (g, ((c + o) % chips) * 2 + h))

    def across(k, o, origin=None):
        block = cent.at[(g if origin is None else origin) + groups * k, h]
        return send(block, block, grp_sem, k, o, (peer(o), d))

    def forward(k, o):
        block = cent.at[peer(o) + groups * k, h]
        return send(block, block, fwd_sem, k, o, (g, partner))

    def if_held(k, o, f):
        if groups * (k + 1) <= rounds:
            f()
        else:
            pl.when(peer(o) + groups * k < rounds)(f)

    def start_slot(k):
        def f():
            gather(k, 1 - h, out_half)
            if k == 0:
                pl.semaphore_wait(barrier, devs - 1 + groups - 1)
            to_partner(k).start()
            gather(k, h, own_half)
            to_partner(k).wait_recv()
            both = own_half[k] + pin[k]
            half[k] = both.reshape(chips, piece, width)
            for o in range(1, chips):
                scatter(k, o).start()

        if_held(k, 0, f)

    for k in range(slots):
        start_slot(k)

    ones_row = jnp.ones((8, width), jnp.bfloat16)

    def row_norms(first, last):
        @pl.loop(first, last)
        def _(t):
            for j in range(WIDE // TILE):
                high, low = split_square(ef[pl.ds(pl.multiple_of(t * WIDE + j * TILE, TILE), TILE), :])
                total = lax.dot_general(ones_row, high, NT, preferred_element_type=jnp.float32)
                total += lax.dot_general(ones_row, low, NT, preferred_element_type=jnp.float32)
                for q in range(TILE // 128):
                    at = t * (WIDE // 128) + j * (TILE // 128) + q
                    rn[at] = total[:, q * 128 : (q + 1) * 128]

    def reduce_chips(k):
        def f():
            total = half[k, c]
            for o in range(1, chips):
                scatter(k, o).wait_recv()
                total += zin[k, o]
            cent[g + groups * k, h, c] = total
            for o in range(1, chips):
                spread(k, o).start()

        if_held(k, 0, f)

    def share(k):
        def f():
            for o in range(1, chips):
                spread(k, o).wait_recv()
            for o in range(1, groups):
                across(k, o).start()
            forward(k, 0).start()

        if_held(k, 0, f)

    steps = rows // WIDE
    parts_of = [steps * i // (slots + 1) for i in range(slots + 2)]
    for k in range(slots):
        row_norms(parts_of[k], parts_of[k + 1])
        reduce_chips(k)
    row_norms(parts_of[slots], steps)
    for k in range(slots):
        share(k)

    ones_col = jnp.ones((width, 128), jnp.bfloat16)

    def compute(r):
        centers = cent[r].reshape(seeds, width)
        high, low = split_square(centers.astype(jnp.float32))
        norms = jnp.dot(high, ones_col, preferred_element_type=jnp.float32)
        norms += jnp.dot(low, ones_col, preferred_element_type=jnp.float32)
        snb[...] = 0.5 * norms

        @pl.loop(0, rows // WIDE)
        def _(t):
            for j in range(WIDE // TILE):
                at = pl.multiple_of(t * WIDE + j * TILE, TILE)
                products = lax.dot_general(
                    cent[r].reshape(seeds, width), e[pl.ds(at, TILE), :], NT,
                    preferred_element_type=jnp.float32,
                )
                for q in range(TILE // 128):
                    score = products[:, q * 128 : (q + 1) * 128] - snb[...]
                    hm[r, t * (WIDE // 128) + j * (TILE // 128) + q] = jnp.max(
                        score.reshape(seeds // 8, 8, 128), axis=0
                    )

    items = [(k, 0) for k in range(slots)]
    items += [(k, o) for k in range(slots) for o in range(1, groups)]

    def relay(k, o):
        def f():
            across(k, o, peer(o)).wait_recv()
            forward(k, o).start()

        if o:
            if_held(k, o, f)

    def finish(k, o):
        def f():
            forward(k, o).wait_recv()
            compute(peer(o) + groups * k)

        if_held(k, o, f)

    for n, (k, o) in enumerate(items):
        if n == slots:
            relay(k, o)
        if n >= slots and n + 1 < len(items):
            relay(*items[n + 1])
        finish(k, o)

    current = prior[...]
    norms = jnp.max(rn[...], axis=1)
    sums = []
    for r in range(rounds):
        best = jnp.max(hm[r], axis=1)
        gap = jnp.maximum(norms - 2.0 * best, 0.0) * (1.0 / width)
        current = jnp.minimum(current, gap)
        sums.append(jnp.sum(current, axis=0, keepdims=True))
    if rounds < 8:
        sums.append(jnp.zeros((8 - rounds, 128), jnp.float32))
    part[...] = jnp.concatenate(sums, axis=0)
    dist[...] = current

    def send_part(o):
        return send(part, parts.at[o], mean_sem, 0, o, (g, (d + o) % devs))

    for o in range(1, devs):
        send_part(o).start()
    total = part[...]
    for o in range(1, devs):
        send_part(o).wait_recv()
        total += parts[o]
    means[...] = jnp.broadcast_to(
        jnp.sum(total, axis=1, keepdims=True) / float(rows * devs), (8, 128)
    )

    for o in range(1, devs):
        send_part(o).wait_send()
    for k in range(slots):
        def drain(k=k):
            to_partner(k).wait_send()
            for o in range(1, chips):
                scatter(k, o).wait_send()
                spread(k, o).wait_send()
            for o in range(1, groups):
                across(k, o).wait_send()

        if_held(k, 0, drain)
        for o in range(groups):
            if_held(k, o, lambda k=k, o=o: forward(k, o).wait_send())


def body(embeddings, prior_dist, seed_ids):
    rows, width = embeddings.shape
    rounds, seeds = seed_ids.shape
    groups, devs = lax.axis_size("grp"), lax.axis_size("dev")
    chips = devs // 2
    slots = (rounds + groups - 1) // groups
    half_rows = seeds // 2
    piece = half_rows // chips
    bf16, f32 = jnp.bfloat16, jnp.float32
    vmem = pl.BlockSpec(memory_space=pltpu.VMEM)
    dist, means = pl.pallas_call(
        functools.partial(kernel, (groups, devs, rounds, seeds, rows, width)),
        out_shape=(
            jax.ShapeDtypeStruct((rows // 128, 128), f32),
            jax.ShapeDtypeStruct((8, 128), f32),
        ),
        in_specs=[
            pl.BlockSpec(memory_space=pltpu.SMEM),
            vmem,
            pl.BlockSpec(memory_space=pl.ANY),
        ],
        out_specs=(vmem, vmem),
        scratch_shapes=[
            pltpu.VMEM((rows, width), bf16),
            pltpu.VMEM((rows + 8, width), f32),
            pltpu.VMEM((half_rows + 8, width), f32),
            pltpu.VMEM((slots, half_rows, width), bf16),
            pltpu.VMEM((slots, half_rows, width), bf16),
            pltpu.VMEM((slots, half_rows, width), bf16),
            pltpu.VMEM((slots, chips, piece, width), bf16),
            pltpu.VMEM((slots, chips, piece, width), bf16),
            pltpu.VMEM((rounds, 2, chips, piece, width), bf16),
            pltpu.VMEM((seeds, 128), f32),
            pltpu.VMEM((rounds, rows // 128, 8, 128), f32),
            pltpu.VMEM((rows // 128, 8, 128), f32),
            pltpu.VMEM((8, 128), f32),
            pltpu.VMEM((devs, 8, 128), f32),
            pltpu.SemaphoreType.DMA((LOAD_CHUNKS,)),
            pltpu.SemaphoreType.DMA((2, slots, 1)),
            pltpu.SemaphoreType.DMA((2, slots, chips)),
            pltpu.SemaphoreType.DMA((2, slots, chips)),
            pltpu.SemaphoreType.DMA((2, slots, groups)),
            pltpu.SemaphoreType.DMA((2, slots, groups)),
            pltpu.SemaphoreType.DMA((2, 1, devs)),
        ],
        compiler_params=pltpu.CompilerParams(
            collective_id=0, has_side_effects=True, vmem_limit_bytes=56 * 1024 * 1024
        ),
        name="seed_rounds",
    )(seed_ids, prior_dist.reshape(rows // 128, 128), embeddings)
    return dist.reshape(rows), means[:rounds, :1]


def solution(mesh):
    placed = (P(("grp", "dev"), None), P(("grp", "dev")), P())
    return jax.shard_map(
        body,
        mesh=mesh,
        in_specs=placed,
        out_specs=(P(("grp", "dev")), P(None, "grp")),
        check_vma=False,
    )
```
